128 devices in a mesh: dp: 32 (over x, y, core), mp: 4 (over z).
Axes of the slice: x: 4, y: 4, z: 4, core: 2. Of those that a mesh axis runs over, the one named last changes fastest.
Arguments:
- grad_parts: bfloat16 [32, 4, 1024, 4096], P('dp', None, None, 'mp'), may hold values from -4000 to 4000
- master: float32 [4, 1024, 4096], P(None, 'dp', 'mp'), may hold values from -6 to 6
- first_moment: float32 [4, 1024, 4096], P(None, 'dp', 'mp'), may hold values from -4 to 4
- second_moment: float32 [4, 1024, 4096], P(None, 'dp', 'mp'), may hold values from 0.25 to 4
- left_basis: bfloat16 [4, 1024, 4096], P(None, 'dp', 'mp'), may hold values from -1 to 1, as said below
- right_basis: bfloat16 [4, 1024, 4096], P(None, 'dp', 'mp'), may hold values from -1 to 1, as said below
Outputs:
- weights: bfloat16 [4, 1024, 4096], P(None, None, 'mp')
- new_master: float32 [4, 1024, 4096], P(None, 'dp', 'mp')
- new_first: float32 [4, 1024, 4096], P(None, 'dp', 'mp')
- new_second: float32 [4, 1024, 4096], P(None, 'dp', 'mp')
The draws below stay inside these ranges and needn't reach their ends.
Inputs may be any that keep to these rules, and one draw needn't show every extreme that they name: Each block left_basis[i, :, j * 1024 : (j + 1) * 1024] is an orthogonal 1024 x 1024 matrix up to rounding. Each block right_basis[i, :, j * 1024 : (j + 1) * 1024] is an orthogonal 1024 x 1024 matrix up to rounding.
All inputs are finite; a program needn't handle non-finite values.
Results may differ from the reference program's by a relative error of at most 0.02.
Values may be sent and summed in bfloat16 or wider, within the bound.
No kernel may reach another device: no remote copies, remote signals or barrier semaphores. Data moves between devices by JAX's collectives and lax.ppermute only.
A program may use at most 128 MiB of HBM per device.

```python
import math
import jax
import jax.numpy as jnp
from jax import lax

D = 4096
BLK = 1024
STEP = 10
NB = 4
N_DP = 32


def orthogonal_blocks(key):
    block_count = D // BLK
    normal_part = jax.random.normal(key, (block_count, block_count, BLK, BLK), jnp.float32)
    factors = jnp.linalg.qr(normal_part)
    return factors[0].transpose(0, 2, 1, 3).reshape(block_count, BLK, D).astype(jnp.bfloat16)


def draw_left_basis(key, part):
    return orthogonal_blocks(jax.random.fold_in(key, 21))


def draw_right_basis(key, part):
    return orthogonal_blocks(jax.random.fold_in(key, 22))


def draw_grad_parts(key, part):
    subkeys = jax.random.split(jax.random.fold_in(key, 11), 5)
    places = jnp.arange(D, dtype=jnp.float32) / D
    row_scale = 10.0 ** (places + 0.3 * jax.random.uniform(subkeys[0], (D,), jnp.float32) - 0.15)
    column_scale = 10.0 ** (places + 0.3 * jax.random.uniform(subkeys[1], (D,), jnp.float32) - 0.15)
    normal_part = jax.random.normal(subkeys[4], (N_DP, D, D), jnp.float32)
    scaled = normal_part * row_scale[None, :, None] * column_scale[None, None, :]
    return scaled.reshape(N_DP, D // BLK, BLK, D).astype(jnp.bfloat16)


def level_of(stream_key, extent, cuts, least, top_value):
    factor_of = 1.0
    for position, blocks in cuts:
        steps = jax.random.uniform(jax.random.fold_in(jax.random.fold_in(stream_key, 6), position), (blocks,), jnp.float32, least / len(cuts), top_value / len(cuts))
        factor_of = factor_of * jnp.repeat(jnp.exp(steps), extent[position] // blocks).reshape((-1,) + (1,) * (len(extent) - 1 - position))
    return factor_of


def scatter_about(rng, shape, width, reach, cuts=(), held_as=jnp.bfloat16):
    entries = jax.random.normal(rng, shape, jnp.float32) * width
    if len(cuts) > 0:
        entries = level_of(rng, shape, cuts, -0.22, 0.18) * entries
    return jnp.clip(entries, min=-reach, max=reach).astype(held_as)


def setup_inputs(seed: int = 0) -> dict:
    splits = jax.random.split(jax.random.key(seed), 7)
    grad_parts = draw_grad_parts(jax.random.fold_in(splits[6], 71), 0)
    master = scatter_about(splits[1], (NB, BLK, D), 1.0, 6.0, ((1, 32), (2, 4)), jnp.float32)
    first_moment = scatter_about(splits[2], (NB, BLK, D), 0.5, 4.0, ((1, 32), (2, 4)), jnp.float32)
    second_moment = jnp.clip(jnp.exp(math.log(4.0) - 2.7725887 * jax.random.uniform(splits[3], (NB, BLK, D), jnp.float32) ** level_of(splits[3], (NB, BLK, D), ((1, 32), (2, 4)), -0.2, 0.2)), 0.25, 4.0)
    left_basis = draw_left_basis(jax.random.fold_in(splits[6], 71), 0)
    right_basis = draw_right_basis(jax.random.fold_in(splits[6], 71), 0)
    return dict(grad_parts=grad_parts, master=master, first_moment=first_moment, second_moment=second_moment, left_basis=left_basis, right_basis=right_basis)


beta_one = 0.95
beta_two = 0.95
epsilon = 1e-08
norm_epsilon = 1e-06
learning_rate = 0.3
decay_rate = 0.1

def reference(grad_parts, master, first_moment, second_moment, left_basis, right_basis):

    def add_part(running_sum, partial_value):
        return (running_sum + partial_value.astype(jnp.float32).reshape(D, D), None)
    gradient, unused_out = lax.scan(add_part, jnp.zeros((D, D), jnp.float32), grad_parts)
    squares_sum = jnp.sum(gradient * gradient)
    clip_scale = jnp.minimum(1.0, 2.0 * D / jnp.sqrt(squares_sum + norm_epsilon))
    grad_low = gradient.astype(jnp.bfloat16)
    master_flat = master.reshape(D, D)
    first_flat = first_moment.reshape(D, D)
    second_flat = second_moment.reshape(D, D)
    left_flat = left_basis.reshape(D, D)
    right_flat = right_basis.reshape(D, D)
    owner_rows = BLK // N_DP
    group_size = N_DP
    block_count = D // BLK
    bias_one = 1.0 - beta_one ** STEP
    bias_two = 1.0 - beta_two ** STEP
    master_rows, first_rows, second_rows = ([], [], [])
    for block_row in range(block_count):
        master_cols, first_cols, second_cols = ([], [], [])
        for block_column in range(block_count):
            row_span = slice(block_row * BLK, (block_row + 1) * BLK)
            column_span = slice(block_column * BLK, (block_column + 1) * BLK)
            grad_block = grad_low[row_span, column_span]
            left_block = left_flat[row_span, column_span]
            right_block = right_flat[row_span, column_span]
            turned = jnp.dot(grad_block.astype(jnp.float32), right_block.astype(jnp.float32), preferred_element_type=jnp.float32).astype(jnp.bfloat16)
            block_terms = jnp.einsum('gra,grb->gab', left_block.reshape(group_size, owner_rows, BLK).astype(jnp.float32), turned.reshape(group_size, owner_rows, BLK).astype(jnp.float32))
            rounded_terms = lax.optimization_barrier(block_terms.astype(jnp.bfloat16))
            rotated = lax.optimization_barrier(jnp.sum(rounded_terms.astype(jnp.float32), axis=0))
            clipped = clip_scale * rotated
            first_new = beta_one * first_flat[row_span, column_span] + (1.0 - beta_one) * clipped
            second_new = beta_two * second_flat[row_span, column_span] + (1.0 - beta_two) * clipped * clipped
            direction = (first_new / bias_one / (jnp.sqrt(second_new / bias_two) + epsilon)).astype(jnp.bfloat16)
            back_rows = jnp.dot(direction.astype(jnp.float32), right_block.T.astype(jnp.float32), preferred_element_type=jnp.float32).astype(jnp.bfloat16)
            update = jnp.dot(left_block.astype(jnp.float32), back_rows.astype(jnp.float32), preferred_element_type=jnp.float32)
            master_new = master_flat[row_span, column_span] * (1.0 - learning_rate * decay_rate) - learning_rate * update
            master_cols.append(master_new)
            first_cols.append(first_new)
            second_cols.append(second_new)
        master_rows.append(jnp.concatenate(master_cols, axis=1))
        first_rows.append(jnp.concatenate(first_cols, axis=1))
        second_rows.append(jnp.concatenate(second_cols, axis=1))
    new_master = jnp.concatenate(master_rows, axis=0).reshape(D // BLK, BLK, D)
    new_first = jnp.concatenate(first_rows, axis=0).reshape(D // BLK, BLK, D)
    new_second = jnp.concatenate(second_rows, axis=0).reshape(D // BLK, BLK, D)
    return (new_master.astype(jnp.bfloat16), new_master, new_first, new_second)
```

```python
import jax
import jax.numpy as jnp
from jax import lax
from jax.sharding import Mesh
from jax.sharding import PartitionSpec as P

D = 4096
STEP = 10
X, Y, CORE, MP = "dp_0", "dp_1", "dp_2", "mp"
DP = (X, Y, CORE)


beta_one = 0.95
beta_two = 0.95
epsilon = 1e-08
norm_epsilon = 1e-06
learning_rate = 0.3
decay_rate = 0.1
bias_one = 1.0 - beta_one**STEP
bias_two = 1.0 - beta_two**STEP


def f32(array):
    return array.astype(jnp.float32)


def low(array):
    return array.astype(jnp.bfloat16)


def shifted(array, axis, step):
    return lax.ppermute(array, axis, [(i, (i + step) % 4) for i in range(4)])


def other_core(array):
    return lax.ppermute(array, CORE, [(0, 1), (1, 0)])


def ring_sum(piece, axis):
    arrived = [shifted(piece(step), axis, step) for step in (1, 3, 2)]
    total = f32(piece(0))
    for term in arrived:
        total = total + f32(term)
    return total


def in_order(pieces, me):
    turned = jnp.stack([pieces[0], pieces[3], pieces[2], pieces[1]] * 2)
    return lax.dynamic_slice_in_dim(turned, lax.rem(4 - me, 4), 4, 0)


def exchange(array, axis, me):
    def piece(step):
        return lax.dynamic_index_in_dim(array, lax.rem(me + step, 4), 0, keepdims=False)

    moved = {step: shifted(piece(step), axis, step) for step in (1, 3, 2)}
    moved[0] = piece(0)
    return in_order(moved, me)


def after(array, value):
    return array + (0.0 * value).astype(array.dtype)


def gradient_rows(parts, x, y, core):
    def by_block(step, side):
        start = (lax.rem(x + step, 4), 0, 0, side, 0, 0)
        return lax.dynamic_slice(parts, start, (1, 2, 4, 1, 32, 1024)).reshape(2, 4, 32, 1024)

    def by_row(step, side):
        start = (0, 2, lax.rem(y + step, 4), side, 0, 0)
        return lax.dynamic_slice(parts, start, (4, 2, 1, 1, 32, 1024)).reshape(4, 2, 32, 1024)

    chip = {}
    for step in (1, 3, 2, 0):
        for name, cut in (("a", by_block), ("b", by_row)):
            mate = other_core(cut(step, 1 - core))
            chip[name, step] = low(f32(cut(step, core)) + f32(mate))
    first = low(ring_sum(lambda step: chip["a", step], X))
    second = low(ring_sum(lambda step: chip["b", step], Y))
    first = ring_sum(
        lambda step: lax.dynamic_index_in_dim(first, lax.rem(y + step, 4), 1, keepdims=False), Y
    )
    second = ring_sum(
        lambda step: lax.dynamic_index_in_dim(second, lax.rem(x + step, 4), 0, keepdims=False), X
    )
    return jnp.concatenate([first, second], 0)


def everywhere(value):
    value = value + other_core(value)
    for axis in (X, Y, MP):
        value = sum((shifted(value, axis, step) for step in (1, 2, 3)), value)
    return value


def per_device(grad_parts, master, first_moment, second_moment, left_basis, right_basis):
    x, y, core = (lax.axis_index(axis) for axis in DP)
    with jax.named_scope("bases"):
        bases = exchange(jnp.stack([right_basis, left_basis], 1), X, x)
        right_rows, left_rows = bases[:, 0], bases[:, 1].reshape(128, 1024)
        right = lax.all_gather(right_rows, (Y, CORE), axis=1, tiled=True).reshape(1024, 1024)
        left = left_rows.reshape(128, 4, 8, 32).swapaxes(1, 2).reshape(128, 1024)
    with jax.named_scope("gradient"):
        gradient = gradient_rows(grad_parts.reshape(4, 4, 4, 2, 32, 1024), x, y, core).reshape(128, 1024)
        grad_low = low(gradient)
    with jax.named_scope("clip"):
        squares = jnp.sum(gradient * gradient, axis=0).reshape(8, 128)
        squares_sum = jnp.sum(everywhere(squares))
        clip_scale = jnp.minimum(1.0, 2.0 * D / jnp.sqrt(squares_sum + norm_epsilon))
    with jax.named_scope("moments"):
        late = f32(grad_low[0, 0])
        moments = exchange(low(after(jnp.stack([first_moment, second_moment], 1), late)), X, x)
    with jax.named_scope("rotate"):
        turned = low(jnp.dot(grad_low, right, preferred_element_type=jnp.float32))
        terms = low(
            lax.dot_general(left, turned, (((0,), (0,)), ((), ())), preferred_element_type=jnp.float32)
        ).reshape(4, 2, 128, 1024)

        def chip_terms(step):
            def cut(side):
                start = (lax.rem(y + step, 4), side, 0, 0)
                return lax.dynamic_slice(terms, start, (1, 1, 128, 1024)).reshape(128, 1024)

            return low(f32(cut(core)) + f32(other_core(cut(1 - core))))

        rotated = ring_sum(chip_terms, Y)
    with jax.named_scope("direction"):
        clipped = clip_scale * rotated
        first_here = beta_one * f32(moments[:, 0].reshape(128, 1024)) + (1.0 - beta_one) * clipped
        second_here = (
            beta_two * f32(moments[:, 1].reshape(128, 1024)) + (1.0 - beta_two) * clipped * clipped
        )
        direction = low(
            first_here / bias_one / (jnp.sqrt(second_here / bias_two) + epsilon)
        )
    with jax.named_scope("back"):
        back = low(
            lax.dot_general(direction, right, (((1,), (1,)), ((), ())), preferred_element_type=jnp.float32)
        )
        column = {step: shifted(back, Y, step) for step in (1, 3, 2)}
        column[0] = back
        update = jnp.zeros((128, 1024), jnp.float32)
        for step in (0, 1, 3, 2):
            mate = other_core(column[step])
            source = lax.rem(y + 4 - step, 4)
            for side, rows in ((core, column[step]), (1 - core, mate)):
                part = lax.dynamic_slice(left, (0, source * 256 + side * 128), (128, 128))
                update = update + jnp.dot(part, rows, preferred_element_type=jnp.float32)
    with jax.named_scope("owners"):
        owned = f32(exchange(low(rotated).reshape(4, 32, 1024), X, x))
        owned = clip_scale * owned
        new_first = beta_one * first_moment + (1.0 - beta_one) * owned
        new_second = beta_two * second_moment + (1.0 - beta_two) * owned * owned
    with jax.named_scope("master"):
        step_rows = f32(exchange(low(update).reshape(4, 32, 1024), X, x))
        new_master = master * (1.0 - learning_rate * decay_rate) - learning_rate * step_rows
        weights = lax.all_gather(low(new_master), DP, axis=1, tiled=True)
    return (weights, new_master, new_first, new_second)


def solution(mesh):
    finer = Mesh(mesh.devices.reshape(4, 4, 2, mesh.shape["mp"]), (X, Y, CORE, MP))
    row_split = P(None, DP, MP)
    return jax.shard_map(
        per_device,
        mesh=finer,
        in_specs=(P(DP, None, None, MP),) + (row_split,) * 5,
        out_specs=(P(None, None, MP),) + (row_split,) * 3,
        check_vma=False,
    )
```

```python
import jax
import jax.numpy as jnp
from jax import lax
from jax.experimental import pallas as pl
from jax.experimental.pallas import tpu as pltpu
from jax.sharding import Mesh
from jax.sharding import PartitionSpec as P

D = 4096
STEP = 10
X, Y, CORE, MP = "dp_0", "dp_1", "dp_2", "mp"
DP = (X, Y, CORE)


beta_one = 0.95
beta_two = 0.95
epsilon = 1e-08
norm_epsilon = 1e-06
learning_rate = 0.3
decay_rate = 0.1
bias_one = 1.0 - beta_one**STEP
bias_two = 1.0 - beta_two**STEP


def f32(array):
    return array.astype(jnp.float32)


def low(array):
    return array.astype(jnp.bfloat16)


def shifted(array, axis, step):
    return lax.ppermute(array, axis, [(i, (i + step) % 4) for i in range(4)])


def other_core(array):
    return lax.ppermute(array, CORE, [(0, 1), (1, 0)])


def ring_sum(piece, axis):
    arrived = [shifted(piece(step), axis, step) for step in (1, 3, 2)]
    total = f32(piece(0))
    for term in arrived:
        total = total + f32(term)
    return total


ANYWHERE = pl.BlockSpec(memory_space=pl.ANY)
SCALARS = pl.BlockSpec(memory_space=pltpu.SMEM)
ON_CHIP = pl.BlockSpec(memory_space=pltpu.VMEM)
COST = pl.CostEstimate(flops=4_000_000, bytes_accessed=2_000_000, transcendentals=0)


def kernel_call(body, inputs, outs, waits=(), scratch=(), kinds=None, room=4):
    def whole(place, *refs):
        body(place, *refs[: len(inputs) - 1], *refs[len(inputs) - 1 + len(waits) :])

    return pl.pallas_call(
        whole,
        out_shape=tuple(jax.ShapeDtypeStruct(shape, dtype) for shape, dtype in outs),
        in_specs=[SCALARS] + list(kinds or [ON_CHIP] * (len(inputs) - 1)) + [ANYWHERE] * len(waits),
        out_specs=tuple(ON_CHIP for _ in outs),
        scratch_shapes=list(scratch),
        cost_estimate=COST,
        compiler_params=pltpu.CompilerParams(vmem_limit_bytes=room * 1024 * 1024),
    )(*inputs, *waits)


def in_order(pieces, me):
    shape, dtype = pieces[0].shape, pieces[0].dtype

    def body(place, *refs):
        for step in range(4):
            refs[4][pl.ds(lax.rem(place[0] + 4 - step, 4), 1)] = refs[step][...][None]

    return kernel_call(
        body, [me.reshape(1)] + [pieces[step] for step in range(4)], [((4,) + shape, dtype)]
    )[0]


HALF = (16, 32, 1024)
ORDER = (1, 3, 2, 0)


def pick_terms(parts, where):
    def body(place, parts_ref, *refs):
        x, y, core = place[0], place[1], place[2]
        for n, step in enumerate(ORDER):
            block, row = lax.rem(x + step, 4), lax.rem(y + step, 4)
            for which, side in ((0, 1 - core), (4, core)):
                out = refs[which + n]

                @pl.loop(0, 4)
                def _(k):
                    for j in range(2):
                        out[2 * k + j] = parts_ref[block, j, k, side]
                        out[8 + 2 * k + j] = parts_ref[k, 2 + j, row, side]

    outs = kernel_call(body, [where, parts], [(HALF, jnp.bfloat16)] * 8, room=24)
    return dict(zip(ORDER, outs[:4])), dict(zip(ORDER, outs[4:]))


def gradient_rows(parts, x, y, core):
    theirs, mine = pick_terms(parts, jnp.stack([x, y, core]))
    by_block, by_row = {}, {}
    for step in ORDER:
        mate = other_core(theirs[step])
        ours = mine[step]
        first = low(f32(ours[:8]) + f32(mate[:8])).reshape(4, 2, 32, 1024)
        second = low(f32(ours[8:]) + f32(mate[8:])).reshape(4, 2, 32, 1024)
        by_block[step] = shifted(first, X, step) if step else first
        by_row[step] = shifted(second, Y, step) if step else second
    first = low(sum((f32(by_block[step]) for step in (1, 3, 2)), f32(by_block[0])))
    second = low(sum((f32(by_row[step]) for step in (1, 3, 2)), f32(by_row[0])))
    terms = []
    for array, axis, me in ((first, Y, y), (second, X, x)):
        pieces = {
            step: lax.dynamic_index_in_dim(array, lax.rem(me + step, 4), 0, keepdims=False)
            for step in ORDER
        }
        terms.append([pieces[0]] + [shifted(pieces[step], axis, step) for step in (1, 3, 2)])

    def body(place, *refs):
        out, squares, acc = refs[8:]
        acc[...] = jnp.zeros((32, 1024), jnp.float32)
        for half in range(2):
            ref = refs[4 * half : 4 * half + 4]
            for j in range(2):
                total = f32(ref[0][j]) + f32(ref[1][j]) + f32(ref[2][j]) + f32(ref[3][j])
                out[2 * half + j] = low(total)
                acc[...] += total * total
        all_rows = acc[0:8] + acc[8:16] + acc[16:24] + acc[24:32]
        tile = sum((all_rows[:, k * 128 : k * 128 + 128] for k in range(1, 8)), all_rows[:, :128])
        squares[...] = jnp.sum(tile, axis=0, keepdims=True)

    return kernel_call(
        body,
        [y.reshape(1)] + terms[0] + terms[1],
        [((4, 32, 1024), jnp.bfloat16), ((1, 128), jnp.float32)],
        scratch=[pltpu.VMEM((32, 1024), jnp.float32)],
    )


def everywhere(value):
    rows = jnp.broadcast_to(value, (128, 128))
    return jnp.sum(lax.all_to_all(rows, (X, Y, CORE, MP), 0, 0, tiled=True), axis=0)


def spread(fresh, x, y, core):
    halves = fresh[:2], fresh[2:]
    stacks = []
    for half, axis in zip(halves, (X, Y)):
        arrived = {step: shifted(half, axis, step) for step in (1, 3, 2)}
        stacks.append(jnp.stack([half] + [arrived[step] for step in (1, 2, 3)]))
    mine = [
        [stack] + [shifted(stack, axis, step) for step in (1, 2, 3)]
        for stack, axis in zip(stacks, (Y, X))
    ]
    theirs = [[other_core(piece) for piece in pieces] for pieces in mine]

    def body(place, *refs):
        x, y, core = place[0], place[1], place[2]
        out = refs[16]
        for n, side in ((0, core), (8, 1 - core)):
            for outer in range(4):

                @pl.loop(0, 4)
                def _(inner):
                    for j in range(2):
                        i, row = lax.rem(x + 4 - inner, 4), lax.rem(y + 4 - outer, 4)
                        out[i, j, row, side] = refs[n + outer][inner, j]
                        i, row = lax.rem(x + 4 - outer, 4), lax.rem(y + 4 - inner, 4)
                        out[i, 2 + j, row, side] = refs[n + 4 + outer][inner, j]

    return kernel_call(
        body,
        [jnp.stack([x, y, core])] + mine[0] + mine[1] + theirs[0] + theirs[1],
        [((4, 4, 4, 2, 32, 1024), jnp.bfloat16)],
        room=24,
    )[0]


def cut_for(arrays, x, waits, dtype):
    many = len(arrays)

    def body(place, *refs):
        for step in range(4):
            block = lax.rem(place[0] + step, 4)
            for n in range(many):
                refs[many + step][n] = refs[n][pl.ds(block, 1)][0].astype(dtype)

    return kernel_call(
        body, [x.reshape(1)] + list(arrays), [((many, 32, 1024), dtype)] * 4, waits
    )


def moved(pieces, x):
    arrived = {step: shifted(pieces[step], X, step) for step in (1, 3, 2)}
    arrived[0] = pieces[0]
    return in_order(arrived, x)


def whole_step(grad_parts, master, first_moment, second_moment, left_basis, right_basis):
    x, y, core = (lax.axis_index(axis) for axis in DP)
    grad_low, squares = gradient_rows(grad_parts.reshape(4, 4, 4, 2, 32, 1024), x, y, core)
    grad_low = grad_low.reshape(128, 1024)
    bases = moved(cut_for([right_basis, left_basis], x, (), jnp.bfloat16), x)
    right = lax.all_gather(bases[:, 0], (Y, CORE), axis=1, tiled=True).reshape(1024, 1024)
    left = bases[:, 1].reshape(128, 4, 8, 32).swapaxes(1, 2).reshape(128, 1024)
    moments = moved(cut_for([first_moment, second_moment], x, (), jnp.bfloat16), x)
    squares_sum = jnp.sum(everywhere(squares))
    clip_scale = jnp.minimum(1.0, 2.0 * D / jnp.sqrt(squares_sum + norm_epsilon))
    turned = low(jnp.dot(grad_low, right, preferred_element_type=jnp.float32))
    terms = low(
        lax.dot_general(left, turned, (((0,), (0,)), ((), ())), preferred_element_type=jnp.float32)
    ).reshape(4, 2, 128, 1024)
    mate = other_core(lax.dynamic_index_in_dim(terms, 1 - core, 1, keepdims=False))
    own = lax.dynamic_index_in_dim(terms, core, 1, keepdims=False)

    def chip(step):
        at = lax.rem(y + step, 4)
        return low(
            f32(lax.dynamic_index_in_dim(own, at, 0, keepdims=False))
            + f32(lax.dynamic_index_in_dim(mate, at, 0, keepdims=False))
        )

    rotated = ring_sum(chip, Y)
    clipped = clip_scale * rotated
    first_here = beta_one * f32(moments[:, 0].reshape(128, 1024)) + (1.0 - beta_one) * clipped
    second_here = (
        beta_two * f32(moments[:, 1].reshape(128, 1024)) + (1.0 - beta_two) * clipped * clipped
    )
    direction = low(
        first_here / bias_one / (jnp.sqrt(second_here / bias_two) + epsilon)
    )
    back = low(
        lax.dot_general(direction, right, (((1,), (1,)), ((), ())), preferred_element_type=jnp.float32)
    )
    column = {step: shifted(back, Y, step) for step in (1, 3, 2)}
    column[0] = back
    update = jnp.zeros((128, 1024), jnp.float32)
    for step in (0, 1, 3, 2):
        mate = other_core(column[step])
        source = lax.rem(y + 4 - step, 4)
        for side, rows in ((core, column[step]), (1 - core, mate)):
            part = lax.dynamic_slice(left, (0, source * 256 + side * 128), (128, 128))
            update = update + jnp.dot(part, rows, preferred_element_type=jnp.float32)
    owned = moved(cut_for([low(rotated).reshape(4, 32, 1024)], x, (back,), jnp.bfloat16), x)
    owned = clip_scale * f32(owned[:, 0])
    new_first = beta_one * first_moment + (1.0 - beta_one) * owned
    new_second = beta_two * second_moment + (1.0 - beta_two) * owned * owned
    kept = moved(cut_for([master], x, (back,), jnp.float32), x).reshape(128, 1024)
    fresh = low(kept * (1.0 - learning_rate * decay_rate) - learning_rate * update)
    weights = spread(fresh.reshape(4, 32, 1024), x, y, core).reshape(4, 1024, 1024)
    rows = moved(cut_for([low(update).reshape(4, 32, 1024)], x, (fresh,), jnp.bfloat16), x)
    new_master = master * (1.0 - learning_rate * decay_rate) - learning_rate * f32(rows[:, 0])
    return (weights, new_master, new_first, new_second)


def solution(mesh):
    finer = Mesh(mesh.devices.reshape(4, 4, 2, mesh.shape["mp"]), (X, Y, CORE, MP))
    row_split = P(None, DP, MP)
    return jax.shard_map(
        whole_step,
        mesh=finer,
        in_specs=(P(DP, None, None, MP),) + (row_split,) * 5,
        out_specs=(P(None, None, MP),) + (row_split,) * 3,
        check_vma=False,
    )
```
